32 devices in a mesh: ep: 8 (over z, x), rep: 4 (over y, core).
Axes of the slice: x: 2, y: 2, z: 4, core: 2. Of those that a mesh axis runs over, the one named last changes fastest.
Arguments:
- tension: float32 [4096, 512], P(('rep', 'ep')), parts along dimension 0, may hold values from -6 to 6
- tile_dest: int32 [4096], P(('rep', 'ep')), parts along dimension 0, may hold values from 0 to 1023, as said below
- restriction: float32 [8, 64], replicated, may hold values from -0.75 to 0.75
- elem_block: int32 [32768], P(('rep', 'ep')), parts along dimension 0, may hold values from 0 to 1023
- shared_own: int32 [8192], P(('rep', 'ep')), parts along dimension 0, may hold values from 0 to 1023, as said below
- shared_send: int32 [8192], P(('rep', 'ep')), parts along dimension 0, may hold values from 0 to 1023
Outputs:
- quadrature: float32 [8, 32768], P(None, ('rep', 'ep')), parts along dimension 1
The draws below stay inside these ranges and needn't reach their ends.
There are 4 independent parts, one for each index of `rep`. The reference program is written for one: setup_inputs(seed, part) draws one part's arguments, and reference() takes and returns one part's arrays. A program takes and returns all parts, laid end to end along the dimension named above; an argument that names none is the same for every part. Nothing has to cross between parts.
Inputs may be any that keep to these rules, and one draw needn't show every extreme that they name: `tile_dest`: A permutation of the tile positions. The 128 entries of one device name, for each device's block of 128 positions, either exactly 32 positions in it or none. `shared_own`: the 256 entries of one device are distinct.
All inputs are finite; a program needn't handle non-finite values.
Results may differ from the reference program's by a relative error of at most 0.00007.
Values sent between devices are 32-bit elements; how exact they have to be, the bound alone decides.
A program may use at most 64 MiB of HBM per device.

```python
import jax
import jax.numpy as jnp
from jax import lax

TILE_NODES = 512
ELEM_NODES = 64
QUAD = 8
TILE_DEV = 128
SHARED = 256
BLOCKS = 8
CAP = 32
TILES = 1024
ELEM_DEV = 1024
ELEMENTS = 8192
N_EP = 8


def draw_tile_dest(key, part):
    key_one, key_two, key_three, key_four = jax.random.split(key, 4)
    sigma = jax.random.permutation(key_one, N_EP).astype(jnp.int32)
    tau = jax.random.permutation(key_two, N_EP).astype(jnp.int32)
    linked = ((sigma[:, None] + tau[None, :]) % 2 == 0).astype(jnp.int32)
    half_ep = N_EP // 2
    chosen = jnp.argsort(1 - linked, axis=1, stable=True)[:, :half_ep].astype(jnp.int32)
    offsets = (jnp.cumsum(linked, axis=0) - linked) * CAP
    slot_ids = jnp.arange(TILE_DEV, dtype=jnp.int32)
    dst_of = chosen[:, slot_ids // CAP]
    local_pos = jnp.take_along_axis(offsets, dst_of, axis=1) + (slot_ids % CAP)[None, :]
    shuffle_dst = jax.vmap(lambda sub: jax.random.permutation(sub, TILE_DEV))(jax.random.split(key_three, N_EP)).astype(jnp.int32)
    final_pos = shuffle_dst[dst_of, local_pos]
    global_dest = dst_of * TILE_DEV + final_pos
    shuffle_src = jax.vmap(lambda sub: jax.random.permutation(sub, TILE_DEV))(jax.random.split(key_four, N_EP)).astype(jnp.int32)
    dest = jnp.take_along_axis(global_dest, shuffle_src, axis=1)
    return dest.reshape(TILES).astype(jnp.int32)


def draw_shared_own(key, part):
    orders = jax.vmap(lambda sub: jax.random.permutation(sub, ELEM_DEV))(jax.random.split(jax.random.fold_in(key, 7), N_EP))
    return orders[:, :SHARED].reshape(N_EP * SHARED).astype(jnp.int32)


def touch_ends(entries, own_key, least, top_value):
    longest = entries.shape.index(max(entries.shape))
    spots = []
    for shift in (0, 1):
        where = [jax.random.randint(jax.random.fold_in(own_key, axis), (), 0, length) for axis, length in enumerate(entries.shape)]
        where[longest] = (where[longest] + shift) % entries.shape[longest]
        spots.append(tuple(where))
    return entries.at[spots[0]].set(least).at[spots[1]].set(top_value)


def block_scale(key, extent, pieces, low, largest):
    level = 1.0
    for dim, parts in pieces:
        heights = jax.random.uniform(jax.random.fold_in(jax.random.fold_in(key, 6), dim), (parts,), jnp.float32, low / len(pieces), largest / len(pieces))
        level = level * jnp.repeat(jnp.exp(heights), extent[dim] // parts).reshape((-1,) + (1,) * (len(extent) - 1 - dim))
    return level


def centred(key, extent, width, reach, cuts=(), held_as=jnp.bfloat16):
    factor_of = block_scale(key, extent, cuts, -0.22, 0.18) if cuts else 1.0
    values = jax.random.normal(key, extent, jnp.float32) * width * factor_of
    return jnp.minimum(jnp.maximum(values, -reach), reach).astype(held_as)


def setup_inputs(seed: int = 0, part: int = 0) -> dict:
    arg_keys = jax.random.split(jax.random.key(seed), 7)
    part_keys = jax.random.split(jax.random.fold_in(arg_keys[6], part), 7)
    tension = centred(part_keys[0], (TILES, TILE_NODES), 1.0, 6.0, ((0, 8),), jnp.float32)
    tile_dest = draw_tile_dest(jax.random.fold_in(jax.random.fold_in(arg_keys[6], part), 71), part)
    restriction = centred(arg_keys[2], (QUAD, ELEM_NODES), ELEM_NODES ** -0.5, 0.75, (), jnp.float32)
    elem_block = touch_ends(jax.random.randint(part_keys[3], (ELEMENTS,), 0, ELEM_DEV), jax.random.fold_in(part_keys[3], 1), 0, ELEM_DEV - 1).astype(jnp.int32)
    shared_own = draw_shared_own(jax.random.fold_in(jax.random.fold_in(arg_keys[6], part), 71), part)
    shared_send = touch_ends(jax.random.randint(part_keys[5], (N_EP * SHARED,), 0, ELEM_DEV), jax.random.fold_in(part_keys[5], 1), 0, ELEM_DEV - 1).astype(jnp.int32)
    return {"tension": tension, "tile_dest": tile_dest, "restriction": restriction, "elem_block": elem_block, "shared_own": shared_own, "shared_send": shared_send}


def reference(tension, tile_dest, restriction, elem_block, shared_own, shared_send):
    placed = jnp.zeros_like(tension).at[tile_dest].set(tension)
    blocks = placed.reshape(TILES * BLOCKS, ELEM_NODES)
    owner_dev = jnp.arange(ELEMENTS, dtype=jnp.int32) // ELEM_DEV
    source = (owner_dev * ELEM_DEV + elem_block).astype(jnp.int32)
    quad_values = jnp.dot(blocks[source], restriction.T, precision=lax.Precision.HIGHEST, preferred_element_type=jnp.float32)
    device = jnp.arange(N_EP * SHARED, dtype=jnp.int32) // SHARED
    next_dev = (device + 1) % N_EP
    next_send = jnp.roll(shared_send, -SHARED)
    own_rows = (device * ELEM_DEV + shared_own).astype(jnp.int32)
    ghost_rows = (next_dev * ELEM_DEV + next_send).astype(jnp.int32)
    mixed = 0.5 * (quad_values[own_rows] + quad_values[ghost_rows])
    averaged = quad_values.at[own_rows].set(mixed)
    return averaged.T
```

```python
import functools

import jax
import jax.numpy as jnp
from jax import lax
from jax.experimental import pallas as pl
from jax.experimental.pallas import tpu as pltpu
from jax.sharding import PartitionSpec as P

F32 = jnp.float32
BF16 = jnp.bfloat16
I32 = jnp.int32
MINOR = (((1,), (1,)), ((), ()))


def iota(shape, dim):
    return lax.broadcasted_iota(I32, shape, dim)


def pieces(x):
    high = x.astype(BF16)
    rest = x - high.astype(F32)
    mid = rest.astype(BF16)
    low = (rest - mid.astype(F32)).astype(BF16)
    return jnp.concatenate([high, mid, low], axis=1)


def select_rows(onehot, x):
    lanes = x.shape[1]
    got = jnp.dot(onehot, pieces(x), preferred_element_type=F32)
    return got[:, :lanes] + got[:, lanes : 2 * lanes] + got[:, 2 * lanes :]


def lanes_of(x, index):
    return jnp.take_along_axis(x, index, axis=1, mode="promise_in_bounds")


def kernel(
    n, cap, tension, dest, restriction, block, own, send, out,
    outbox, inbox, ghost_out, ghost_in, send_sem, recv_sem, ghost_sem,
):
    me = lax.axis_index("ep")
    tiles = tension.shape[0]
    quad, nodes = restriction.shape
    width = tension.shape[1] // nodes * quad
    lanes = 2 * width
    rows_e = block.shape[0]
    halves = own.shape[0]
    wide = tiles * halves

    barrier = pltpu.get_barrier_semaphore()
    for k in range(1, n):
        pl.semaphore_signal(barrier, inc=1, device_id={"ep": lax.rem(me + k, n)})

    for h in range(halves):
        want = jnp.broadcast_to(send[h : h + 1, :], (rows_e, tiles))
        got = lanes_of(block[...], lax.rem(want, tiles))
        ghost_out[h : h + 1, :] = jnp.sum(
            jnp.where(lax.div(want, tiles) == iota((rows_e, tiles), 0), got, 0),
            axis=0, keepdims=True,
        )

    place = dest[...]
    target = lax.div(place, tiles)
    to_peer = jnp.broadcast_to(target, (n, tiles)) == iota((n, tiles), 0)
    to_peer = to_peer.astype(F32)
    earlier = (iota((tiles, tiles), 0) < iota((tiles, tiles), 1)).astype(F32).astype(BF16)
    before = jnp.dot(to_peer.astype(BF16), earlier, preferred_element_type=F32)
    rank = jnp.sum(before * to_peer, axis=0, keepdims=True).astype(I32)
    slot = target * cap + rank
    slots = n * cap
    pack = (jnp.broadcast_to(slot, (slots, tiles)) == iota((slots, tiles), 0)).astype(F32).astype(BF16)
    at_rank = jnp.broadcast_to(rank, (tiles, tiles)) == lax.rem(iota((tiles, tiles), 0), cap)
    where_to = (to_peer * (lax.rem(place, tiles) + 1).astype(F32)).astype(BF16)
    where_to = lax.dot_general(
        where_to, at_rank.astype(F32).astype(BF16), MINOR, preferred_element_type=F32
    )

    full = (lanes, tension.shape[1])
    weight = jnp.concatenate([restriction[...]] * (full[1] // nodes), axis=1)
    weight = jnp.concatenate([weight] * (lanes // quad), axis=0)
    mine = lax.div(lax.rem(iota(full, 0), width), quad) == lax.div(iota(full, 1), nodes)
    weight = jnp.where(mine, weight, 0.0)
    local = lax.dot_general(
        tension[...], weight, MINOR,
        precision=lax.Precision.HIGHEST, preferred_element_type=F32,
    )
    packed = select_rows(pack, local)
    first = iota((cap, lanes), 1) < width
    for p in range(n):
        after = (p + 1) % n
        outbox[p, :cap, :] = jnp.where(
            first, packed[p * cap : (p + 1) * cap], packed[after * cap : (after + 1) * cap]
        )
        outbox[p, cap : cap + 1, :] = where_to[p : p + 1]
        outbox[p, cap + 1 : cap + 2, :] = where_to[after : after + 1]

    pl.semaphore_wait(barrier, n - 1)
    copies = []
    for k in range(1, n):
        peer = lax.rem(me + k, n)
        copies.append(
            pltpu.make_async_remote_copy(
                src_ref=outbox.at[peer],
                dst_ref=inbox.at[me],
                send_sem=send_sem.at[k],
                recv_sem=recv_sem.at[k],
                device_id={"ep": peer},
            )
        )
    ghosts = pltpu.make_async_remote_copy(
        src_ref=ghost_out,
        dst_ref=ghost_in,
        send_sem=ghost_sem.at[0],
        recv_sem=ghost_sem.at[1],
        device_id={"ep": lax.rem(me + n - 1, n)},
    )
    ghosts.start()
    for copy in copies:
        copy.start()
    inbox[me] = outbox[me]

    owned = jnp.concatenate([own[h : h + 1, :] for h in range(halves)], axis=1)
    entry = (iota((rows_e, wide), 1) + 1).astype(F32)
    entry = jnp.where(
        jnp.broadcast_to(lax.div(owned, tiles), (rows_e, wide)) == iota((rows_e, wide), 0), entry, 0.0
    ).astype(BF16)
    column = jnp.broadcast_to(lax.rem(owned, tiles), (tiles, wide)) == iota((tiles, wide), 0)
    shared = lax.dot_general(
        entry, column.astype(F32).astype(BF16), MINOR, preferred_element_type=F32
    ).astype(I32)

    ghosts.wait()
    for copy in copies:
        copy.wait()

    per = tiles // cap
    lane = lax.div(iota((1, tiles), 1), cap)
    onehot = []
    for which in range(2):
        parts = []
        for h in range(slots // tiles):
            pos = jnp.zeros((1, tiles), F32)
            for s in range(per):
                pos = jnp.where(lane == s, inbox[h * per + s, cap + which : cap + which + 1, :], pos)
            pos = jnp.broadcast_to(pos.astype(I32), (tiles, tiles))
            parts.append((pos == iota((tiles, tiles), 0) + 1).astype(F32).astype(BF16))
        onehot.append(jnp.concatenate(parts, axis=1))
    arrived = jnp.concatenate([inbox[s, :cap, :] for s in range(n)], axis=0)
    placed = select_rows(jnp.concatenate(onehot, axis=0), arrived)
    placed = jnp.where(iota((tiles, lanes), 1) < width, placed[:tiles], placed[tiles:]).T

    def values(index, base):
        index = jnp.broadcast_to(index, (quad, tiles))
        blocks = width // quad
        tile, part = lax.div(index, blocks), lax.rem(index, blocks)
        got = lanes_of(placed[base : base + quad], tile)
        for b in range(1, blocks):
            low = base + b * quad
            got = jnp.where(part == b, lanes_of(placed[low : low + quad], tile), got)
        return got

    ghost = [values(ghost_in[h : h + 1, :], width) for h in range(halves)]
    for r in range(rows_e):
        mine = values(block[r : r + 1, :], 0)
        which = jnp.broadcast_to(shared[r : r + 1, :], (quad, tiles))
        number = jnp.maximum(which - 1, 0)
        other = lanes_of(ghost[0], lax.rem(number, tiles))
        for h in range(1, halves):
            other = jnp.where(
                lax.div(number, tiles) == h, lanes_of(ghost[h], lax.rem(number, tiles)), other
            )
        out[:, r * tiles : (r + 1) * tiles] = jnp.where(which > 0, 0.5 * (mine + other), mine)


def per_device(tension, tile_dest, restriction, elem_block, shared_own, shared_send):
    n = lax.axis_size("ep")
    tiles = tension.shape[0]
    cap = 2 * tiles // n
    quad, nodes = restriction.shape
    lanes = 2 * (tension.shape[1] // nodes * quad)
    halves = shared_own.shape[0] // tiles
    vmem = pl.BlockSpec(memory_space=pltpu.VMEM)
    return pl.pallas_call(
        functools.partial(kernel, n, cap),
        out_shape=jax.ShapeDtypeStruct((quad, elem_block.shape[0]), F32),
        in_specs=[vmem] * 6,
        out_specs=vmem,
        scratch_shapes=[
            pltpu.VMEM((n, cap + 2, lanes), F32),
            pltpu.VMEM((n, cap + 2, lanes), F32),
            pltpu.VMEM((halves, tiles), I32),
            pltpu.VMEM((halves, tiles), I32),
            pltpu.SemaphoreType.DMA((n,)),
            pltpu.SemaphoreType.DMA((n,)),
            pltpu.SemaphoreType.DMA((2,)),
        ],
        compiler_params=pltpu.CompilerParams(collective_id=0, has_side_effects=True),
    )(
        tension,
        tile_dest.reshape(1, tiles),
        restriction,
        elem_block.reshape(-1, tiles),
        shared_own.reshape(halves, tiles),
        shared_send.reshape(halves, tiles),
    )


def solution(mesh):
    return jax.shard_map(
        per_device,
        mesh=mesh,
        in_specs=(
            P(("rep", "ep"), None),
            P(("rep", "ep")),
            P(),
            P(("rep", "ep")),
            P(("rep", "ep")),
            P(("rep", "ep")),
        ),
        out_specs=P(None, ("rep", "ep")),
        check_vma=False,
    )
```

```python
import functools

import jax
import jax.numpy as jnp
from jax import lax
from jax.experimental import pallas as pl
from jax.experimental.pallas import tpu as pltpu
from jax.sharding import PartitionSpec as P

F32 = jnp.float32
BF16 = jnp.bfloat16
I32 = jnp.int32
MINOR = (((1,), (1,)), ((), ()))


def iota(shape, dim):
    return lax.broadcasted_iota(I32, shape, dim)


def pieces(x):
    high = x.astype(BF16)
    return high, (x - high.astype(F32)).astype(BF16)


def select_rows(onehot, x):
    lanes = x.shape[1]
    got = jnp.dot(onehot, jnp.concatenate(pieces(x), axis=1), preferred_element_type=F32)
    return got[:, :lanes] + got[:, lanes:]


def lanes_of(x, index):
    return jnp.take_along_axis(x, index, axis=1, mode="promise_in_bounds")


def partner(me, k, n):
    if True:
        return lax.rem(me + k, n)
    bit, peer = 1, 0
    while bit < n:
        have = lax.rem(me // bit, 2)
        peer = peer + bit * (1 - have if k & bit else have)
        bit *= 2
    return peer


def kernel(
    n, cap, *refs
):
    given, out, held = refs[:6], refs[6], refs[7:13]
    outbox, inbox, ghost_out, ghost_in, load_sem, send_sem, recv_sem, ghost_sem = refs[13:]
    dest, send, block, restriction, own, tension = held
    me = lax.axis_index("ep")
    tiles = tension.shape[0]
    quad, nodes = restriction.shape
    width = tension.shape[1] // nodes * quad
    lanes = 2 * width
    rows_e = block.shape[0]
    halves = own.shape[0]
    wide = tiles * halves

    barrier = pltpu.get_barrier_semaphore()
    for k in range(1, n):
        pl.semaphore_signal(barrier, inc=1, device_id={"ep": partner(me, n - k, n)})

    arrive = [pltpu.make_async_copy(a, b, load_sem.at[i]) for i, (a, b) in enumerate(zip(given, held))]
    for copy in arrive:
        copy.start()

    arrive[1].wait()
    arrive[2].wait()
    for h in range(halves):
        want = jnp.broadcast_to(send[h : h + 1, :], (rows_e, tiles))
        got = lanes_of(block[...], lax.rem(want, tiles))
        ghost_out[h : h + 1, :] = jnp.sum(
            jnp.where(lax.div(want, tiles) == iota((rows_e, tiles), 0), got, 0),
            axis=0, keepdims=True,
        )

    arrive[0].wait()
    place = dest[...]
    target = lax.div(place, tiles)
    to_peer = jnp.broadcast_to(target, (n, tiles)) == iota((n, tiles), 0)
    to_peer = to_peer.astype(F32)
    earlier = (iota((tiles, tiles), 0) < iota((tiles, tiles), 1)).astype(F32).astype(BF16)
    before = jnp.dot(to_peer.astype(BF16), earlier, preferred_element_type=F32)
    rank = jnp.sum(before * to_peer, axis=0, keepdims=True).astype(I32)
    slot = target * cap + rank
    slots = n * cap
    pack = (jnp.broadcast_to(slot, (slots, tiles)) == iota((slots, tiles), 0)).astype(F32).astype(BF16)
    at_rank = jnp.broadcast_to(rank, (tiles, tiles)) == lax.rem(iota((tiles, tiles), 0), cap)
    where_to = (to_peer * (lax.rem(place, tiles) + 1).astype(F32)).astype(BF16)
    where_to = lax.dot_general(
        where_to, at_rank.astype(F32).astype(BF16), MINOR, preferred_element_type=F32
    )

    full = (lanes, tension.shape[1])
    arrive[3].wait()
    weight = jnp.concatenate([restriction[...]] * (full[1] // nodes), axis=1)
    weight = jnp.concatenate([weight] * (lanes // quad), axis=0)
    mine = lax.div(lax.rem(iota(full, 0), width), quad) == lax.div(iota(full, 1), nodes)
    weight = jnp.where(mine, weight, 0.0)
    arrive[5].wait()
    nodal, nodal_low = pieces(tension[...])
    weight, weight_low = pieces(weight)
    by = functools.partial(lax.dot_general, dimension_numbers=MINOR, preferred_element_type=F32)
    local = by(nodal, weight) + (by(nodal_low, weight) + by(nodal, weight_low))
    packed = select_rows(pack, local)
    first = iota((cap, lanes), 1) < width
    for p in range(n):
        after = (p + 1) % n
        outbox[p, :cap, :] = jnp.where(
            first, packed[p * cap : (p + 1) * cap], packed[after * cap : (after + 1) * cap]
        )
        outbox[p, cap : cap + 1, :] = where_to[p : p + 1]
        outbox[p, cap + 1 : cap + 2, :] = where_to[after : after + 1]

    pl.semaphore_wait(barrier, n - 1)
    copies = []
    for k in range(1, n):
        peer = partner(me, k, n)
        copies.append(
            pltpu.make_async_remote_copy(
                src_ref=outbox.at[peer],
                dst_ref=inbox.at[me],
                send_sem=send_sem.at[k],
                recv_sem=recv_sem.at[k],
                device_id={"ep": peer},
            )
        )
    ghosts = pltpu.make_async_remote_copy(
        src_ref=ghost_out,
        dst_ref=ghost_in,
        send_sem=ghost_sem.at[0],
        recv_sem=ghost_sem.at[1],
        device_id={"ep": lax.rem(me + n - 1, n)},
    )
    ghosts.start()
    for copy in copies:
        copy.start()
    inbox[me] = outbox[me]

    arrive[4].wait()
    owned = jnp.concatenate([own[h : h + 1, :] for h in range(halves)], axis=1)
    entry = (iota((rows_e, wide), 1) + 1).astype(F32)
    entry = jnp.where(
        jnp.broadcast_to(lax.div(owned, tiles), (rows_e, wide)) == iota((rows_e, wide), 0), entry, 0.0
    ).astype(BF16)
    column = jnp.broadcast_to(lax.rem(owned, tiles), (tiles, wide)) == iota((tiles, wide), 0)
    shared = lax.dot_general(
        entry, column.astype(F32).astype(BF16), MINOR, preferred_element_type=F32
    ).astype(I32)

    ghosts.wait()
    for copy in copies:
        copy.wait()

    per = tiles // cap
    lane = lax.div(iota((1, tiles), 1), cap)
    onehot = []
    for which in range(2):
        parts = []
        for h in range(slots // tiles):
            pos = jnp.zeros((1, tiles), F32)
            for s in range(per):
                pos = jnp.where(lane == s, inbox[h * per + s, cap + which : cap + which + 1, :], pos)
            pos = jnp.broadcast_to(pos.astype(I32), (tiles, tiles))
            parts.append((pos == iota((tiles, tiles), 0) + 1).astype(F32).astype(BF16))
        onehot.append(jnp.concatenate(parts, axis=1))
    arrived = jnp.concatenate([inbox[s, :cap, :] for s in range(n)], axis=0)
    placed = select_rows(jnp.concatenate(onehot, axis=0), arrived)
    placed = jnp.where(iota((tiles, lanes), 1) < width, placed[:tiles], placed[tiles:]).T

    def values(index, base):
        index = jnp.broadcast_to(index, (quad, tiles))
        blocks = width // quad
        tile, part = lax.div(index, blocks), lax.rem(index, blocks)
        got = lanes_of(placed[base : base + quad], tile)
        for b in range(1, blocks):
            low = base + b * quad
            got = jnp.where(part == b, lanes_of(placed[low : low + quad], tile), got)
        return got

    ghost = [values(ghost_in[h : h + 1, :], width) for h in range(halves)]
    for r in range(rows_e):
        mine = values(block[r : r + 1, :], 0)
        which = jnp.broadcast_to(shared[r : r + 1, :], (quad, tiles))
        number = jnp.maximum(which - 1, 0)
        other = lanes_of(ghost[0], lax.rem(number, tiles))
        for h in range(1, halves):
            other = jnp.where(
                lax.div(number, tiles) == h, lanes_of(ghost[h], lax.rem(number, tiles)), other
            )
        out[:, r * tiles : (r + 1) * tiles] = jnp.where(which > 0, 0.5 * (mine + other), mine)


def per_device(tension, tile_dest, restriction, elem_block, shared_own, shared_send):
    n = lax.axis_size("ep")
    tiles = tension.shape[0]
    cap = 2 * tiles // n
    quad, nodes = restriction.shape
    lanes = 2 * (tension.shape[1] // nodes * quad)
    halves = shared_own.shape[0] // tiles
    given = (
        tile_dest.reshape(1, tiles),
        shared_send.reshape(halves, tiles),
        elem_block.reshape(-1, tiles),
        restriction,
        shared_own.reshape(halves, tiles),
        tension,
    )
    return pl.pallas_call(
        functools.partial(kernel, n, cap),
        out_shape=jax.ShapeDtypeStruct((quad, elem_block.shape[0]), F32),
        in_specs=[pl.BlockSpec(memory_space=pltpu.HBM)] * 6,
        out_specs=pl.BlockSpec(memory_space=pltpu.VMEM),
        scratch_shapes=[pltpu.VMEM(a.shape, a.dtype) for a in given]
        + [
            pltpu.VMEM((n, cap + 2, lanes), F32),
            pltpu.VMEM((n, cap + 2, lanes), F32),
            pltpu.VMEM((halves, tiles), I32),
            pltpu.VMEM((halves, tiles), I32),
            pltpu.SemaphoreType.DMA((6,)),
            pltpu.SemaphoreType.DMA((n,)),
            pltpu.SemaphoreType.DMA((n,)),
            pltpu.SemaphoreType.DMA((2,)),
        ],
        compiler_params=pltpu.CompilerParams(
            collective_id=0, has_side_effects=True, vmem_limit_bytes=60 * 1024 * 1024
        ),
    )(*given)


def solution(mesh):
    return jax.shard_map(
        per_device,
        mesh=mesh,
        in_specs=(
            P(("rep", "ep"), None),
            P(("rep", "ep")),
            P(),
            P(("rep", "ep")),
            P(("rep", "ep")),
            P(("rep", "ep")),
        ),
        out_specs=P(None, ("rep", "ep")),
        check_vma=False,
    )
```

```python
import functools

import jax
import jax.numpy as jnp
from jax import lax
from jax.experimental import pallas as pl
from jax.experimental.pallas import tpu as pltpu
from jax.sharding import PartitionSpec as P

F32 = jnp.float32
BF16 = jnp.bfloat16
I32 = jnp.int32
MINOR = (((1,), (1,)), ((), ()))


def iota(shape, dim):
    return lax.broadcasted_iota(I32, shape, dim)


def pieces(x):
    high = x.astype(BF16)
    return high, (x - high.astype(F32)).astype(BF16)


def select_rows(onehot, x):
    lanes = x.shape[1]
    got = jnp.dot(onehot, jnp.concatenate(pieces(x), axis=1), preferred_element_type=F32)
    return got[:, :lanes] + got[:, lanes:]


def lanes_of(x, index):
    return jnp.take_along_axis(x, index, axis=1, mode="promise_in_bounds")


def partner(me, k, n):
    if True:
        return lax.rem(me + k, n)
    bit, peer = 1, 0
    while bit < n:
        have = lax.rem(me // bit, 2)
        peer = peer + bit * (1 - have if k & bit else have)
        bit *= 2
    return peer


def kernel(
    n, cap, *refs
):
    given, out, held = refs[:6], refs[6], refs[7:13]
    outbox, inbox, ghost_out, ghost_in, load_sem, send_sem, recv_sem, ghost_sem = refs[13:]
    dest, send, block, restriction, own, tension = held
    me = lax.axis_index("ep")
    tiles = tension.shape[0]
    quad, nodes = restriction.shape
    width = tension.shape[1] // nodes * quad
    lanes = 2 * width
    rows_e = block.shape[0]
    halves = own.shape[0]
    wide = tiles * halves

    barrier = pltpu.get_barrier_semaphore()
    for k in range(1, n):
        pl.semaphore_signal(barrier, inc=1, device_id={"ep": partner(me, n - k, n)})

    arrive = [pltpu.make_async_copy(a, b, load_sem.at[i]) for i, (a, b) in enumerate(zip(given, held))]
    for i in (5, 0, 3, 1, 2, 4):
        arrive[i].start()

    arrive[0].wait()
    arrive[3].wait()
    arrive[5].wait()
    place = dest[...]
    target = lax.div(place, tiles)
    to_peer = jnp.broadcast_to(target, (n, tiles)) == iota((n, tiles), 0)
    to_peer = to_peer.astype(F32)
    earlier = (iota((tiles, tiles), 0) < iota((tiles, tiles), 1)).astype(F32).astype(BF16)
    before = jnp.dot(to_peer.astype(BF16), earlier, preferred_element_type=F32)
    rank = jnp.sum(before * to_peer, axis=0, keepdims=True).astype(I32)
    slot = target * cap + rank
    slots = n * cap
    pack = (jnp.broadcast_to(slot, (slots, tiles)) == iota((slots, tiles), 0)).astype(F32).astype(BF16)
    at_rank = jnp.broadcast_to(rank, (tiles, tiles)) == lax.rem(iota((tiles, tiles), 0), cap)
    where_to = (to_peer * (lax.rem(place, tiles) + 1).astype(F32)).astype(BF16)
    where_to = lax.dot_general(
        where_to, at_rank.astype(F32).astype(BF16), MINOR, preferred_element_type=F32
    )

    full = (lanes, tension.shape[1])
    weight = jnp.concatenate([restriction[...]] * (full[1] // nodes), axis=1)
    weight = jnp.concatenate([weight] * (lanes // quad), axis=0)
    mine = lax.div(lax.rem(iota(full, 0), width), quad) == lax.div(iota(full, 1), nodes)
    weight = jnp.where(mine, weight, 0.0)
    nodal, nodal_low = pieces(tension[...])
    weight, weight_low = pieces(weight)
    by = functools.partial(lax.dot_general, dimension_numbers=MINOR, preferred_element_type=F32)
    local = by(nodal, weight) + (by(nodal_low, weight) + by(nodal, weight_low))
    packed = select_rows(pack, local)
    first = iota((cap, lanes), 1) < width
    for p in range(n):
        after = (p + 1) % n
        outbox[p, :cap, :] = jnp.where(
            first, packed[p * cap : (p + 1) * cap], packed[after * cap : (after + 1) * cap]
        )
        outbox[p, cap : cap + 1, :] = where_to[p : p + 1]
        outbox[p, cap + 1 : cap + 2, :] = where_to[after : after + 1]

    pl.semaphore_wait(barrier, n - 1)
    copies = []
    for k in range(1, n):
        peer = partner(me, k, n)
        copies.append(
            pltpu.make_async_remote_copy(
                src_ref=outbox.at[peer],
                dst_ref=inbox.at[me],
                send_sem=send_sem.at[k],
                recv_sem=recv_sem.at[k],
                device_id={"ep": peer},
            )
        )
    for copy in copies:
        copy.start()
    arrive[1].wait()
    arrive[2].wait()
    for h in range(halves):
        want = jnp.broadcast_to(send[h : h + 1, :], (rows_e, tiles))
        got = lanes_of(block[...], lax.rem(want, tiles))
        ghost_out[h : h + 1, :] = jnp.sum(
            jnp.where(lax.div(want, tiles) == iota((rows_e, tiles), 0), got, 0),
            axis=0, keepdims=True,
        )
    ghosts = pltpu.make_async_remote_copy(
        src_ref=ghost_out,
        dst_ref=ghost_in,
        send_sem=ghost_sem.at[0],
        recv_sem=ghost_sem.at[1],
        device_id={"ep": lax.rem(me + n - 1, n)},
    )
    ghosts.start()
    inbox[me] = outbox[me]

    arrive[4].wait()
    owned = jnp.concatenate([own[h : h + 1, :] for h in range(halves)], axis=1)
    entry = (iota((rows_e, wide), 1) + 1).astype(F32)
    entry = jnp.where(
        jnp.broadcast_to(lax.div(owned, tiles), (rows_e, wide)) == iota((rows_e, wide), 0), entry, 0.0
    ).astype(BF16)
    column = jnp.broadcast_to(lax.rem(owned, tiles), (tiles, wide)) == iota((tiles, wide), 0)
    shared = lax.dot_general(
        entry, column.astype(F32).astype(BF16), MINOR, preferred_element_type=F32
    ).astype(I32)

    ghosts.wait()
    for copy in copies:
        copy.wait()

    per = tiles // cap
    lane = lax.div(iota((1, tiles), 1), cap)
    onehot = []
    for which in range(2):
        parts = []
        for h in range(slots // tiles):
            pos = jnp.zeros((1, tiles), F32)
            for s in range(per):
                pos = jnp.where(lane == s, inbox[h * per + s, cap + which : cap + which + 1, :], pos)
            pos = jnp.broadcast_to(pos.astype(I32), (tiles, tiles))
            parts.append((pos == iota((tiles, tiles), 0) + 1).astype(F32).astype(BF16))
        onehot.append(jnp.concatenate(parts, axis=1))
    arrived = jnp.concatenate([inbox[s, :cap, :] for s in range(n)], axis=0)
    placed = select_rows(jnp.concatenate(onehot, axis=0), arrived)
    placed = jnp.where(iota((tiles, lanes), 1) < width, placed[:tiles], placed[tiles:]).T

    def values(index, base):
        index = jnp.broadcast_to(index, (quad, tiles))
        blocks = width // quad
        tile, part = lax.div(index, blocks), lax.rem(index, blocks)
        got = lanes_of(placed[base : base + quad], tile)
        for b in range(1, blocks):
            low = base + b * quad
            got = jnp.where(part == b, lanes_of(placed[low : low + quad], tile), got)
        return got

    ghost = [values(ghost_in[h : h + 1, :], width) for h in range(halves)]
    for r in range(rows_e):
        mine = values(block[r : r + 1, :], 0)
        which = jnp.broadcast_to(shared[r : r + 1, :], (quad, tiles))
        number = jnp.maximum(which - 1, 0)
        other = lanes_of(ghost[0], lax.rem(number, tiles))
        for h in range(1, halves):
            other = jnp.where(
                lax.div(number, tiles) == h, lanes_of(ghost[h], lax.rem(number, tiles)), other
            )
        out[:, r * tiles : (r + 1) * tiles] = jnp.where(which > 0, 0.5 * (mine + other), mine)


def per_device(tension, tile_dest, restriction, elem_block, shared_own, shared_send):
    n = lax.axis_size("ep")
    tiles = tension.shape[0]
    cap = 2 * tiles // n
    quad, nodes = restriction.shape
    lanes = 2 * (tension.shape[1] // nodes * quad)
    halves = shared_own.shape[0] // tiles
    given = (
        tile_dest.reshape(1, tiles),
        shared_send.reshape(halves, tiles),
        elem_block.reshape(-1, tiles),
        restriction,
        shared_own.reshape(halves, tiles),
        tension,
    )
    return pl.pallas_call(
        functools.partial(kernel, n, cap),
        out_shape=jax.ShapeDtypeStruct((quad, elem_block.shape[0]), F32),
        in_specs=[pl.BlockSpec(memory_space=pltpu.HBM)] * 6,
        out_specs=pl.BlockSpec(memory_space=pltpu.VMEM),
        scratch_shapes=[pltpu.VMEM(a.shape, a.dtype) for a in given]
        + [
            pltpu.VMEM((n, cap + 2, lanes), F32),
            pltpu.VMEM((n, cap + 2, lanes), F32),
            pltpu.VMEM((halves, tiles), I32),
            pltpu.VMEM((halves, tiles), I32),
            pltpu.SemaphoreType.DMA((6,)),
            pltpu.SemaphoreType.DMA((n,)),
            pltpu.SemaphoreType.DMA((n,)),
            pltpu.SemaphoreType.DMA((2,)),
        ],
        compiler_params=pltpu.CompilerParams(
            collective_id=0, has_side_effects=True, vmem_limit_bytes=16 * 2**20
        ),
    )(*[pltpu.with_memory_space_constraint(a, pltpu.HBM) for a in given])


def solution(mesh):
    return jax.shard_map(
        per_device,
        mesh=mesh,
        in_specs=(
            P(("rep", "ep"), None),
            P(("rep", "ep")),
            P(),
            P(("rep", "ep")),
            P(("rep", "ep")),
            P(("rep", "ep")),
        ),
        out_specs=P(None, ("rep", "ep")),
        check_vma=False,
    )
```

```python
import functools

import jax
import jax.numpy as jnp
from jax import lax
from jax.experimental import pallas as pl
from jax.experimental.pallas import tpu as pltpu
from jax.sharding import PartitionSpec as P

F32 = jnp.float32
BF16 = jnp.bfloat16
I32 = jnp.int32
MINOR = (((1,), (1,)), ((), ()))


def iota(shape, dim):
    return lax.broadcasted_iota(I32, shape, dim)


def pieces(x):
    high = x.astype(BF16)
    return high, (x - high.astype(F32)).astype(BF16)


def select_rows(onehot, x):
    lanes = x.shape[1]
    got = jnp.dot(onehot, jnp.concatenate(pieces(x), axis=1), preferred_element_type=F32)
    return got[:, :lanes] + got[:, lanes:]


def lanes_of(x, index):
    return jnp.take_along_axis(x, index, axis=1, mode="promise_in_bounds")


def partner(me, k, n):
    if True:
        return lax.rem(me + k, n)
    bit, peer = 1, 0
    while bit < n:
        have = lax.rem(me // bit, 2)
        peer = peer + bit * (1 - have if k & bit else have)
        bit *= 2
    return peer


def kernel(
    n, cap, *refs
):
    given, out, held = refs[:6], refs[6], refs[7:13]
    outbox, inbox, ghost_out, ghost_in, load_sem, send_sem, recv_sem, ghost_sem = refs[13:]
    dest, send, block, restriction, own, tension = held
    me = lax.axis_index("ep")
    tiles = tension.shape[0]
    quad, nodes = restriction.shape
    width = tension.shape[1] // nodes * quad
    lanes = 2 * width
    rows_e = block.shape[0]
    halves = own.shape[0]
    wide = tiles * halves

    barrier = pltpu.get_barrier_semaphore()
    for k in range(1, n):
        pl.semaphore_signal(barrier, inc=1, device_id={"ep": partner(me, n - k, n)})

    arrive = [pltpu.make_async_copy(a, b, load_sem.at[i]) for i, (a, b) in enumerate(zip(given, held))]
    for i in (5, 0, 3, 1, 2, 4):
        arrive[i].start()

    arrive[0].wait()
    arrive[3].wait()
    arrive[5].wait()
    place = dest[...]
    target = lax.div(place, tiles)
    to_peer = jnp.broadcast_to(target, (n, tiles)) == iota((n, tiles), 0)
    to_peer = to_peer.astype(F32)
    earlier = (iota((tiles, tiles), 0) < iota((tiles, tiles), 1)).astype(F32).astype(BF16)
    before = jnp.dot(to_peer.astype(BF16), earlier, preferred_element_type=F32)
    rank = jnp.sum(before * to_peer, axis=0, keepdims=True).astype(I32)
    slot = target * cap + rank
    slots = n * cap
    pack = (jnp.broadcast_to(slot, (slots, tiles)) == iota((slots, tiles), 0)).astype(F32).astype(BF16)
    at_rank = jnp.broadcast_to(rank, (tiles, tiles)) == lax.rem(iota((tiles, tiles), 0), cap)
    where_to = (to_peer * (lax.rem(place, tiles) + 1).astype(F32)).astype(BF16)
    where_to = lax.dot_general(
        where_to, at_rank.astype(F32).astype(BF16), MINOR, preferred_element_type=F32
    )

    full = (lanes, tension.shape[1])
    weight = jnp.concatenate([restriction[...]] * (full[1] // nodes), axis=1)
    weight = jnp.concatenate([weight] * (lanes // quad), axis=0)
    mine = lax.div(lax.rem(iota(full, 0), width), quad) == lax.div(iota(full, 1), nodes)
    weight = jnp.where(mine, weight, 0.0)
    nodal, nodal_low = pieces(tension[...])
    weight, weight_low = pieces(weight)
    by = functools.partial(lax.dot_general, dimension_numbers=MINOR, preferred_element_type=F32)
    local = by(nodal, weight) + (by(nodal_low, weight) + by(nodal, weight_low))
    packed = select_rows(pack, local)
    first = iota((cap, lanes), 1) < width
    for p in range(n):
        after = (p + 1) % n
        outbox[p, :cap, :] = jnp.where(
            first, packed[p * cap : (p + 1) * cap], packed[after * cap : (after + 1) * cap]
        )
        outbox[p, cap : cap + 1, :] = where_to[p : p + 1]
        outbox[p, cap + 1 : cap + 2, :] = where_to[after : after + 1]

    pl.semaphore_wait(barrier, n - 1)
    copies = []
    for k in range(1, n):
        peer = partner(me, k, n)
        copies.append(
            pltpu.make_async_remote_copy(
                src_ref=outbox.at[peer],
                dst_ref=inbox.at[me],
                send_sem=send_sem.at[k],
                recv_sem=recv_sem.at[k],
                device_id={"ep": peer},
            )
        )
    for copy in copies:
        copy.start()
    arrive[1].wait()
    arrive[2].wait()
    for h in range(halves):
        want = jnp.broadcast_to(send[h : h + 1, :], (rows_e, tiles))
        got = lanes_of(block[...], lax.rem(want, tiles))
        ghost_out[h : h + 1, :] = jnp.sum(
            jnp.where(lax.div(want, tiles) == iota((rows_e, tiles), 0), got, 0),
            axis=0, keepdims=True,
        )
    ghosts = pltpu.make_async_remote_copy(
        src_ref=ghost_out,
        dst_ref=ghost_in,
        send_sem=ghost_sem.at[0],
        recv_sem=ghost_sem.at[1],
        device_id={"ep": lax.rem(me + n - 1, n)},
    )
    ghosts.start()
    inbox[me] = outbox[me]

    arrive[4].wait()
    owned = jnp.concatenate([own[h : h + 1, :] for h in range(halves)], axis=1)
    entry = (iota((rows_e, wide), 1) + 1).astype(F32)
    entry = jnp.where(
        jnp.broadcast_to(lax.div(owned, tiles), (rows_e, wide)) == iota((rows_e, wide), 0), entry, 0.0
    ).astype(BF16)
    column = jnp.broadcast_to(lax.rem(owned, tiles), (tiles, wide)) == iota((tiles, wide), 0)
    shared = lax.dot_general(
        entry, column.astype(F32).astype(BF16), MINOR, preferred_element_type=F32
    ).astype(I32)

    blocks = width // quad
    own_tile, own_part = lax.div(block[...], blocks), lax.rem(block[...], blocks)
    number = jnp.maximum(shared - 1, 0)
    ghost_half, ghost_lane = lax.div(number, tiles), lax.rem(number, tiles)

    ghosts.wait()
    ghost_tile, ghost_part = lax.div(ghost_in[...], blocks), lax.rem(ghost_in[...], blocks)
    for copy in copies:
        copy.wait()

    per = tiles // cap
    lane = lax.div(iota((1, tiles), 1), cap)
    onehot = []
    for which in range(2):
        parts = []
        for h in range(slots // tiles):
            pos = jnp.zeros((1, tiles), F32)
            for s in range(per):
                pos = jnp.where(lane == s, inbox[h * per + s, cap + which : cap + which + 1, :], pos)
            pos = jnp.broadcast_to(pos.astype(I32), (tiles, tiles))
            parts.append((pos == iota((tiles, tiles), 0) + 1).astype(F32).astype(BF16))
        onehot.append(jnp.concatenate(parts, axis=1))
    arrived = jnp.concatenate([inbox[s, :cap, :] for s in range(n)], axis=0)
    placed = select_rows(jnp.concatenate(onehot, axis=0), arrived)
    placed = jnp.where(iota((tiles, lanes), 1) < width, placed[:tiles], placed[tiles:]).T

    def spread(x, row):
        return jnp.broadcast_to(x[row : row + 1, :], (quad, tiles))

    def values(tile, part, base):
        got = lanes_of(placed[base : base + quad], tile)
        for b in range(1, blocks):
            low = base + b * quad
            got = jnp.where(part == b, lanes_of(placed[low : low + quad], tile), got)
        return got

    ghost = [values(spread(ghost_tile, h), spread(ghost_part, h), width) for h in range(halves)]
    for r in range(rows_e):
        mine = values(spread(own_tile, r), spread(own_part, r), 0)
        other = lanes_of(ghost[0], spread(ghost_lane, r))
        for h in range(1, halves):
            other = jnp.where(spread(ghost_half, r) == h, lanes_of(ghost[h], spread(ghost_lane, r)), other)
        out[:, r * tiles : (r + 1) * tiles] = jnp.where(
            spread(shared, r) > 0, 0.5 * (mine + other), mine
        )


def per_device(tension, tile_dest, restriction, elem_block, shared_own, shared_send):
    n = lax.axis_size("ep")
    tiles = tension.shape[0]
    cap = 2 * tiles // n
    quad, nodes = restriction.shape
    lanes = 2 * (tension.shape[1] // nodes * quad)
    halves = shared_own.shape[0] // tiles
    given = (
        tile_dest.reshape(1, tiles),
        shared_send.reshape(halves, tiles),
        elem_block.reshape(-1, tiles),
        restriction,
        shared_own.reshape(halves, tiles),
        tension,
    )
    return pl.pallas_call(
        functools.partial(kernel, n, cap),
        out_shape=jax.ShapeDtypeStruct((quad, elem_block.shape[0]), F32),
        in_specs=[pl.BlockSpec(memory_space=pltpu.HBM)] * 6,
        out_specs=pl.BlockSpec(memory_space=pltpu.VMEM),
        scratch_shapes=[pltpu.VMEM(a.shape, a.dtype) for a in given]
        + [
            pltpu.VMEM((n, cap + 2, lanes), F32),
            pltpu.VMEM((n, cap + 2, lanes), F32),
            pltpu.VMEM((halves, tiles), I32),
            pltpu.VMEM((halves, tiles), I32),
            pltpu.SemaphoreType.DMA((6,)),
            pltpu.SemaphoreType.DMA((n,)),
            pltpu.SemaphoreType.DMA((n,)),
            pltpu.SemaphoreType.DMA((2,)),
        ],
        compiler_params=pltpu.CompilerParams(
            collective_id=0, has_side_effects=True, vmem_limit_bytes=16 * 2**20
        ),
    )(*[pltpu.with_memory_space_constraint(a, pltpu.HBM) for a in given])


def solution(mesh):
    return jax.shard_map(
        per_device,
        mesh=mesh,
        in_specs=(
            P(("rep", "ep"), None),
            P(("rep", "ep")),
            P(),
            P(("rep", "ep")),
            P(("rep", "ep")),
            P(("rep", "ep")),
        ),
        out_specs=P(None, ("rep", "ep")),
        check_vma=False,
    )
```
